256 devices in a mesh: row: 32 (over z, x_hi, core), col: 8 (over x_lo, y).
Axes of the slice: x: 4 (x_hi: 2, x_lo: 2; x = x_hi * 2 + x_lo), y: 4, z: 8, core: 2. Of those that a mesh axis runs over, the one named last changes fastest.
Arguments:
- coefficients: float32 [2, 1, 256, 256, 256], P(None, None, 'col', 'row'), may hold values from -6 to 6
- real_bands: float32 [8, 256, 256, 256], P(None, 'col', 'row'), may hold values from -6 to 6
Outputs:
- spline_coefs: float32 [2, 1, 256, 256, 256], P(None, None, None, ('row', 'col'))
- spline_table: float32 [8, 256, 256, 256], P('col', 'row')
The draws below stay inside these ranges and needn't reach their ends.
All inputs are finite; a program needn't handle non-finite values.
Results may differ from the reference program's by a relative error of at most 0.00007.
Values sent between devices are 32-bit elements; how exact they have to be, the bound alone decides.
No kernel may reach another device: no remote copies, remote signals or barrier semaphores. Data moves between devices by JAX's collectives and lax.ppermute only.
A program may use at most 64 MiB of HBM per device.

```python
import jax
import jax.numpy as jnp
from jax import lax

NX = 256
NY = 256
NZ = 256
NB = 1
NA = 8


def block_levels(own_key, extent, split, low, top_value):
    def one(axis_at, parts):
        draws = jax.random.uniform(jax.random.fold_in(jax.random.fold_in(own_key, 6), axis_at), (parts,), jnp.float32, low / len(split), top_value / len(split))
        return jnp.repeat(jnp.exp(draws), extent[axis_at] // parts).reshape((-1,) + (1,) * (len(extent) - axis_at - 1))

    gain = one(*split[0])
    for cut in split[1:]:
        gain = gain * one(*cut)
    return gain


def noise(own_key, dims, deviation, bound, split=(), kind=jnp.bfloat16):
    drawn = jax.random.normal(own_key, dims, jnp.float32) * deviation
    if len(split) > 0:
        drawn = block_levels(own_key, dims, split, -0.22, 0.18) * drawn
    return jnp.clip(drawn, min=-bound, max=bound).astype(kind)


def setup_inputs(seed: int = 0) -> dict:
    streams_of = jax.random.split(jax.random.key(seed), 3)
    return {
        "coefficients": noise(streams_of[0], (2, NB, NZ, NY, NX), 1.0, 6.0, ((2, 8), (3, 32)), jnp.float32),
        "real_bands": noise(streams_of[1], (NA, NZ, NY, NX), 1.0, 6.0, ((1, 8), (2, 32)), jnp.float32),
    }


def prefilter(length, dtype):
    angle = (2.0 * jnp.pi / length) * jnp.arange(length).astype(dtype)
    return (4.0 + 2.0 * jnp.cos(angle)) / 6.0


def reference(coefficients, real_bands):
    dtype = coefficients.dtype
    scale = prefilter(NZ, dtype)[:, None, None] * prefilter(NY, dtype)[None, :, None] * prefilter(NX, dtype)[None, None, :]

    def one_band(pair):
        spectrum = (pair[0] + 1j * pair[1]) / scale
        field = jnp.fft.ifftn(spectrum, axes=(0, 1, 2), norm="ortho")
        field = jnp.transpose(field, (0, 2, 1))
        return jnp.stack([jnp.real(field), jnp.imag(field)]).astype(dtype)

    moved = lax.map(one_band, (coefficients[0], coefficients[1]))
    spline_coefs = jnp.transpose(moved, (1, 0, 2, 3, 4))
    spline_table = jnp.transpose(real_bands, (0, 3, 2, 1))
    return spline_coefs, spline_table
```

```python
import functools

import jax
import jax.numpy as jnp
import ml_dtypes
import numpy as np
from jax import lax
from jax.experimental import pallas as pl
from jax.experimental.pallas import tpu as pltpu
from jax.sharding import PartitionSpec as P

N = 256
ROWS, COLS = 32, 8
ZL, YL, XL = N // COLS, N // ROWS, N // ROWS
BANDS = 8
PIECE = 20
LANES = 128
f32 = jnp.float32
bf16 = jnp.bfloat16


@functools.cache
def tables():
    k = np.arange(N)
    angle = 2.0 * np.pi * ((k[:, None] * k[None, :]) % N) / N
    weight = 6.0 / ((4.0 + 2.0 * np.cos(2.0 * np.pi * k / N)) * np.sqrt(N))
    both = np.concatenate([np.cos(angle) * weight[None, :], np.sin(angle) * weight[None, :]])
    by_rest = both.reshape(2 * N, ROWS, YL).swapaxes(1, 2).reshape(2 * N, N)
    out = []
    for whole in (both, by_rest):
        high = whole.astype(ml_dtypes.bfloat16)
        low = (whole - high.astype(np.float64)).astype(ml_dtypes.bfloat16)
        out += [high, low]
    return tuple(out)


def split(value):
    high = value.astype(bf16)
    return high, (value - high.astype(f32)).astype(bf16)


def product(w_high, w_low, value, dims):
    high, low = split(value)

    def one(left, right):
        return lax.dot_general(left, right, (dims, ((), ())), preferred_element_type=f32)

    return one(w_high, high) + (one(w_high, low) + one(w_low, high))


def exchange_blocks(vs):
    lane = lax.broadcasted_iota(jnp.int32, (8, LANES), 1)
    low = lane < 64
    even = (lane & 32) == 0
    u = list(vs)
    for i in (0, 1):
        a, b = u[i], u[i + 2]
        u[i] = jnp.where(low, a, pltpu.roll(b, 64, 1))
        u[i + 2] = jnp.where(low, pltpu.roll(a, 64, 1), b)
    for i in (0, 2):
        a, b = u[i], u[i + 1]
        u[i] = jnp.where(even, a, pltpu.roll(b, 32, 1))
        u[i + 1] = jnp.where(even, pltpu.roll(a, 96, 1), b)
    return u


def pack(coef_ref, bands_ref, wh_ref, wl_ref, out_ref, cbuf, buf, spec, sems):
    halves = [pl.ds(h * LANES, LANES) for h in range(2)]
    starts = [pltpu.make_async_copy(coef_ref.at[:, halves[h]], cbuf.at[h], sems.at[h]) for h in range(2)]
    copies = [
        [pltpu.make_async_copy(bands_ref.at[b, :, halves[h]], buf.at[b, h], sems.at[2 + 2 * b + h]) for h in range(2)]
        for b in range(BANDS)
    ]
    for copy in starts + sum(copies, []):
        copy.start()
    for copy in starts:
        copy.wait()
    rows = [
        jnp.concatenate([cbuf[h, pl.ds(part * N + y, ZL, stride=YL), :] for h in range(2)], axis=1)
        for part in range(2)
        for y in range(YL)
    ]
    q = product(wh_ref[...], wl_ref[...], jnp.concatenate(rows), ((1,), (1,)))
    for h in range(2):
        one, two = (slice(p * N + h * LANES, p * N + (h + 1) * LANES) for p in range(2))
        spec[h, pl.ds(0, N), :] = q[:N, one] - q[N:, two]
        spec[h, pl.ds(N, N), :] = q[N:, one] + q[:N, two]
    for b in range(BANDS):
        base = b * ROWS * PIECE
        for xh in range(2):
            copies[b][xh].wait()
            for yh in range(2):
                block = jnp.concatenate([buf[b, xh, pl.ds(yh * 4 + k, ZL, stride=YL), :] for k in range(4)])
                turned = block.T
                for r in range(16):
                    row = base + PIECE * (xh * 16 + r) + 8 * yh
                    out_ref[pl.ds(row, 8), :] = turned[r * 8 : r * 8 + 8]
        for part in range(2):
            for yh in range(2):
                for g in range(ROWS // 8):
                    out_ref[pl.ds(base + PIECE * 8 * g + 16 + part * 2 + yh, 8, stride=PIECE), :] = spec[
                        yh, pl.ds(part * N + g * 64 + b, 8, stride=8), :
                    ]


GROUPS = 4


def unpack(in_ref, yh_ref, yl_ref, wh_ref, wl_ref, coefs_ref, table_ref, tab, field, sems):
    flat = tab.reshape(2, XL * N, LANES)
    size = N // GROUPS
    copies = []
    for group in range(GROUPS):
        for h in range(2):
            for r in range(group * ROWS // GROUPS, (group + 1) * ROWS // GROUPS):
                for yh in range(2):
                    vs = [in_ref[pl.ds(PIECE * ((h * 4 + c) * ROWS + r) + 8 * yh, 8), :] for c in range(4)]
                    for k, v in enumerate(exchange_blocks(vs)):
                        flat[h, pl.ds(r * YL + yh * 4 + k, XL, stride=N), :] = v
            where = pl.ds(group * size, size)
            copies.append(
                pltpu.make_async_copy(
                    tab.at[h, :, where, :],
                    table_ref.at[:, where, pl.ds(h * LANES, LANES)],
                    sems.at[2 * group + h],
                )
            )
            copies[-1].start()
    for part in range(2):
        for yh in range(2):
            for g in range(ROWS // 8):
                for h in range(2):
                    vs = [
                        in_ref[
                            pl.ds(PIECE * ((h * 4 + c) * ROWS + g * 8) + 16 + part * 2 + yh, 8, stride=PIECE), :
                        ]
                        for c in range(4)
                    ]
                    for k, v in enumerate(exchange_blocks(vs)):
                        field[pl.ds((yh * 4 + k) * ROWS + g * 8, 8), pl.ds(part * N + h * LANES, LANES)] = v
    q = product(yh_ref[...], yl_ref[...], field[...], ((1,), (0,)))
    along = jnp.concatenate([q[:N, :N] - q[N:, N:], q[N:, :N] + q[:N, N:]])
    q = product(wh_ref[...], wl_ref[...], along, ((1,), (1,)))
    real = q[:N, :N] - q[N:, N:]
    imag = q[N:, :N] + q[:N, N:]
    for h in range(2):
        lanes = slice(h * LANES, (h + 1) * LANES)
        coefs_ref[pl.ds(h, N, stride=2), :] = real[:, lanes]
        coefs_ref[pl.ds(2 * N + h, N, stride=2), :] = imag[:, lanes]
    for copy in copies:
        copy.wait()


vmem = pl.BlockSpec(memory_space=pltpu.VMEM)
anywhere = pl.BlockSpec(memory_space=pltpu.HBM)


def local(coefficients, real_bands):
    assert coefficients.shape == (2, 1, ZL, YL, N)
    assert real_bands.shape == (BANDS, ZL, YL, N)
    assert (lax.axis_size("row"), lax.axis_size("col")) == (ROWS, COLS)
    wh, wl, yh, yl = (jnp.asarray(t) for t in tables())
    total = ROWS * COLS * PIECE
    packed = pl.pallas_call(
        pack,
        name="pack",
        out_shape=jax.ShapeDtypeStruct((total, LANES), f32),
        in_specs=[anywhere, anywhere, vmem, vmem],
        out_specs=vmem,
        scratch_shapes=[
            pltpu.VMEM((2, 2 * ZL * YL, LANES), f32),
            pltpu.VMEM((BANDS, 2, ZL * YL, LANES), f32),
            pltpu.VMEM((2, 2 * N, LANES), f32),
            pltpu.SemaphoreType.DMA((2 + 2 * BANDS,)),
        ],
        compiler_params=pltpu.CompilerParams(vmem_limit_bytes=24 << 20),
    )(coefficients.reshape(2 * ZL * YL, N), real_bands.reshape(BANDS, ZL * YL, N), wh, wl)
    packed = packed.reshape(ROWS * COLS, PIECE // 4, 4, LANES)
    got = lax.all_to_all(packed, ("col", "row"), split_axis=0, concat_axis=0, tiled=True)
    coefs, table = pl.pallas_call(
        unpack,
        name="unpack",
        out_shape=[
            jax.ShapeDtypeStruct((4 * N, LANES), f32),
            jax.ShapeDtypeStruct((XL, N, N), f32),
        ],
        in_specs=[vmem] * 5,
        out_specs=[vmem, anywhere],
        scratch_shapes=[
            pltpu.VMEM((2, XL, N, LANES), f32),
            pltpu.VMEM((N, 2 * N), f32),
            pltpu.SemaphoreType.DMA((2 * GROUPS,)),
        ],
        compiler_params=pltpu.CompilerParams(vmem_limit_bytes=24 << 20),
    )(got.reshape(total, LANES), yh, yl, wh, wl)
    return coefs.reshape(2, 1, N, 1, N), table.reshape(1, XL, N, N)


def solution(mesh):
    placed = (P(None, None, "col", "row", None), P(None, "col", "row", None))
    return jax.shard_map(
        local,
        mesh=mesh,
        in_specs=placed,
        out_specs=(P(None, None, None, ("row", "col"), None), P("col", "row", None, None)),
        check_vma=False,
    )
```

```python
import functools

import jax
import jax.numpy as jnp
import ml_dtypes
import numpy as np
from jax import lax
from jax.experimental import pallas as pl
from jax.experimental.pallas import tpu as pltpu
from jax.sharding import PartitionSpec as P

N = 256
ROWS, COLS = 32, 8
ZL, YL, XL = N // COLS, N // ROWS, N // ROWS
BANDS = 8
PIECE = 20
LANES = 128
f32 = jnp.float32
bf16 = jnp.bfloat16


@functools.cache
def tables():
    k = np.arange(N)
    angle = 2.0 * np.pi * ((k[:, None] * k[None, :]) % N) / N
    weight = 6.0 / ((4.0 + 2.0 * np.cos(2.0 * np.pi * k / N)) * np.sqrt(N))
    both = np.concatenate([np.cos(angle) * weight[None, :], np.sin(angle) * weight[None, :]])
    by_rest = both.reshape(2 * N, ROWS, YL).swapaxes(1, 2).reshape(2 * N, N)
    out = []
    for whole in (both, by_rest):
        high = whole.astype(ml_dtypes.bfloat16)
        low = (whole - high.astype(np.float64)).astype(ml_dtypes.bfloat16)
        out += [high, low]
    return tuple(out)


def split(value):
    high = value.astype(bf16)
    return high, (value - high.astype(f32)).astype(bf16)


def product(w_high, w_low, value, dims):
    high, low = split(value)

    def one(left, right):
        return lax.dot_general(left, right, (dims, ((), ())), preferred_element_type=f32)

    return one(w_high, high) + (one(w_high, low) + one(w_low, high))


def exchange_blocks(vs):
    lane = lax.broadcasted_iota(jnp.int32, (8, LANES), 1)
    low = lane < 64
    even = (lane & 32) == 0
    u = list(vs)
    for i in (0, 1):
        a, b = u[i], u[i + 2]
        u[i] = jnp.where(low, a, pltpu.roll(b, 64, 1))
        u[i + 2] = jnp.where(low, pltpu.roll(a, 64, 1), b)
    for i in (0, 2):
        a, b = u[i], u[i + 1]
        u[i] = jnp.where(even, a, pltpu.roll(b, 32, 1))
        u[i + 1] = jnp.where(even, pltpu.roll(a, 96, 1), b)
    return u


def pack(coef_ref, bands_ref, wh_hbm, wl_hbm, out_ref, cbuf, buf, wh_ref, wl_ref, spec, sems):
    halves = [pl.ds(h * LANES, LANES) for h in range(2)]
    starts = [pltpu.make_async_copy(coef_ref.at[:, halves[h]], cbuf.at[h], sems.at[h]) for h in range(2)]
    starts += [
        pltpu.make_async_copy(wh_hbm, wh_ref, sems.at[2 + 2 * BANDS]),
        pltpu.make_async_copy(wl_hbm, wl_ref, sems.at[3 + 2 * BANDS]),
    ]
    copies = [
        [pltpu.make_async_copy(bands_ref.at[b, :, halves[h]], buf.at[b, h], sems.at[2 + 2 * b + h]) for h in range(2)]
        for b in range(BANDS)
    ]
    for copy in starts + sum(copies, []):
        copy.start()
    def turn(b):
        for xh in range(2):
            for yh in range(2):
                block = jnp.concatenate([buf[b, xh, pl.ds(yh * 4 + k, ZL, stride=YL), :] for k in range(4)])
                turned = block.T
                for r in range(16):
                    row = b * ROWS * PIECE + PIECE * (xh * 16 + r) + 8 * yh
                    out_ref[pl.ds(row, 8), :] = turned[r * 8 : r * 8 + 8]

    def wait(bands):
        for b in bands:
            for copy in copies[b]:
                copy.wait()

    for step, bands in enumerate(STEPS):
        wait(bands)
        if step == DFT_AT:
            for copy in starts:
                copy.wait()
            rows = [
                jnp.concatenate([cbuf[h, pl.ds(part * N + y, ZL, stride=YL), :] for h in range(2)], axis=1)
                for part in range(2)
                for y in range(YL)
            ]
            q = product(wh_ref[...], wl_ref[...], jnp.concatenate(rows), ((1,), (1,)))
            for h in range(2):
                one, two = (slice(p * N + h * LANES, p * N + (h + 1) * LANES) for p in range(2))
                spec[h, pl.ds(0, N), :] = q[:N, one] - q[N:, two]
                spec[h, pl.ds(N, N), :] = q[N:, one] + q[:N, two]
        for b in bands:
            turn(b)
    for b in range(BANDS):
        for part in range(2):
            for yh in range(2):
                for g in range(ROWS // 8):
                    out_ref[pl.ds(b * ROWS * PIECE + PIECE * 8 * g + 16 + part * 2 + yh, 8, stride=PIECE), :] = spec[
                        yh, pl.ds(part * N + g * 64 + b, 8, stride=8), :
                    ]


EDGES = (0, 8, 16, 24, 32)
TRANSFORM_AT = 0
STEPS = ((0, 1, 2, 3), (4, 5, 6, 7))
DFT_AT = 0


def unpack(in_ref, yh_ref, yl_ref, wh_ref, wl_ref, coefs_ref, table_ref, cout, tab, field, sems):
    flat = tab.reshape(2, XL * (N + 8), LANES)
    copies = []

    def transform():
        for part in range(2):
            for yh in range(2):
                for g in range(ROWS // 8):
                    for h in range(2):
                        vs = [
                            in_ref[
                                pl.ds(PIECE * ((h * 4 + c) * ROWS + g * 8) + 16 + part * 2 + yh, 8, stride=PIECE), :
                            ]
                            for c in range(4)
                        ]
                        for k, v in enumerate(exchange_blocks(vs)):
                            field[pl.ds((yh * 4 + k) * ROWS + g * 8, 8), pl.ds(part * N + h * LANES, LANES)] = v
        q = product(yh_ref[...], yl_ref[...], field[...], ((1,), (0,)))
        along = jnp.concatenate([q[:N, :N] - q[N:, N:], q[N:, :N] + q[:N, N:]])
        q = product(wh_ref[...], wl_ref[...], along, ((1,), (1,)))
        real = q[:N, :N] - q[N:, N:]
        imag = q[N:, :N] + q[:N, N:]
        for h in range(2):
            lanes = slice(h * LANES, (h + 1) * LANES)
            cout[pl.ds(h, N, stride=2), :] = real[:, lanes]
            cout[pl.ds(2 * N + h, N, stride=2), :] = imag[:, lanes]
        copies.append(pltpu.make_async_copy(cout, coefs_ref, sems.at[2 * len(EDGES)]))
        copies[-1].start()

    for group, (first, last) in enumerate(zip(EDGES[:-1], EDGES[1:])):
        if group == TRANSFORM_AT:
            transform()
        for h in range(2):
            for r in range(first, last):
                for yh in range(2):
                    vs = [in_ref[pl.ds(PIECE * ((h * 4 + c) * ROWS + r) + 8 * yh, 8), :] for c in range(4)]
                    for k, v in enumerate(exchange_blocks(vs)):
                        flat[h, pl.ds(r * YL + yh * 4 + k, XL, stride=N + 8), :] = v
            where = pl.ds(first * YL, (last - first) * YL)
            copies.append(
                pltpu.make_async_copy(
                    tab.at[h, :, where, :],
                    table_ref.at[:, where, pl.ds(h * LANES, LANES)],
                    sems.at[2 * group + h],
                )
            )
            copies[-1].start()
    if TRANSFORM_AT == len(EDGES) - 1:
        transform()
    for copy in copies:
        copy.wait()


vmem = pl.BlockSpec(memory_space=pltpu.VMEM)
anywhere = pl.BlockSpec(memory_space=pltpu.HBM)


def local(coefficients, real_bands):
    assert coefficients.shape == (2, 1, ZL, YL, N)
    assert real_bands.shape == (BANDS, ZL, YL, N)
    assert (lax.axis_size("row"), lax.axis_size("col")) == (ROWS, COLS)
    wh, wl, yh, yl = (jnp.asarray(t) for t in tables())
    total = ROWS * COLS * PIECE
    packed = pl.pallas_call(
        pack,
        name="pack",
        out_shape=jax.ShapeDtypeStruct((total, LANES), f32),
        in_specs=[anywhere] * 4,
        out_specs=vmem,
        scratch_shapes=[
            pltpu.VMEM((2, 2 * ZL * YL, LANES), f32),
            pltpu.VMEM((BANDS, 2, ZL * YL, LANES), f32),
            pltpu.VMEM((2 * N, N), bf16),
            pltpu.VMEM((2 * N, N), bf16),
            pltpu.VMEM((2, 2 * N, LANES), f32),
            pltpu.SemaphoreType.DMA((4 + 2 * BANDS,)),
        ],
        compiler_params=pltpu.CompilerParams(vmem_limit_bytes=24 << 20),
    )(
        pltpu.with_memory_space_constraint(coefficients.reshape(2 * ZL * YL, N), pltpu.HBM),
        pltpu.with_memory_space_constraint(real_bands.reshape(BANDS, ZL * YL, N), pltpu.HBM),
        pltpu.with_memory_space_constraint(wh, pltpu.HBM),
        pltpu.with_memory_space_constraint(wl, pltpu.HBM),
    )
    packed = packed.reshape(ROWS * COLS, PIECE // 4, 4, LANES)
    got = lax.all_to_all(packed, ("col", "row"), split_axis=0, concat_axis=0, tiled=True)
    coefs, table = pl.pallas_call(
        unpack,
        name="unpack",
        out_shape=[
            jax.ShapeDtypeStruct((4 * N, LANES), f32),
            jax.ShapeDtypeStruct((XL, N, N), f32),
        ],
        in_specs=[vmem] * 5,
        out_specs=[anywhere, anywhere],
        scratch_shapes=[
            pltpu.VMEM((4 * N, LANES), f32),
            pltpu.VMEM((2, XL, N + 8, LANES), f32),
            pltpu.VMEM((N, 2 * N), f32),
            pltpu.SemaphoreType.DMA((2 * len(EDGES) + 1,)),
        ],
        compiler_params=pltpu.CompilerParams(vmem_limit_bytes=24 << 20),
    )(got.reshape(total, LANES), yh, yl, wh, wl)
    return coefs.reshape(2, 1, N, 1, N), table.reshape(1, XL, N, N)


def solution(mesh):
    placed = (P(None, None, "col", "row", None), P(None, "col", "row", None))
    return jax.shard_map(
        local,
        mesh=mesh,
        in_specs=placed,
        out_specs=(P(None, None, None, ("row", "col"), None), P("col", "row", None, None)),
        check_vma=False,
    )
```

```python
import functools

import jax
import jax.numpy as jnp
import ml_dtypes
import numpy as np
from jax import lax
from jax.experimental import pallas as pl
from jax.experimental.pallas import tpu as pltpu
from jax.sharding import PartitionSpec as P

N = 256
ROWS, COLS = 32, 8
ZL, YL, XL = N // COLS, N // ROWS, N // ROWS
BANDS = 8
ZD, PLANE = 8, 32
PIECE = 10 * PLANE
SLOT = 10 * ZD
LANES = 128
f32 = jnp.float32
bf16 = jnp.bfloat16


@functools.cache
def tables():
    k = np.arange(N)
    angle = 2.0 * np.pi * ((k[:, None] * k[None, :]) % N) / N
    weight = 6.0 / ((4.0 + 2.0 * np.cos(2.0 * np.pi * k / N)) * np.sqrt(N))
    both = np.concatenate([np.cos(angle) * weight[None, :], np.sin(angle) * weight[None, :]])
    by_rest = both.reshape(2 * N, ZD, ROWS // ZD, YL).swapaxes(1, 2).reshape(2 * N, N)
    out = []
    for whole in (both, by_rest):
        high = whole.astype(ml_dtypes.bfloat16)
        low = (whole - high.astype(np.float64)).astype(ml_dtypes.bfloat16)
        out += [high, low]
    return tuple(out)


def split(value):
    high = value.astype(bf16)
    return high, (value - high.astype(f32)).astype(bf16)


def product(w_high, w_low, value, dims):
    high, low = split(value)

    def one(left, right):
        return lax.dot_general(left, right, (dims, ((), ())), preferred_element_type=f32)

    return one(w_high, high) + (one(w_high, low) + one(w_low, high))


def exchange_blocks(vs):
    lane = lax.broadcasted_iota(jnp.int32, vs[0].shape, 1)
    low = lane < 64
    even = (lane & 32) == 0
    out = []
    for q in range(4):
        a, b, c, d = (vs[(place - q) % 4] for place in range(4))
        u = jnp.where(low, jnp.where(even, a, b), jnp.where(even, c, d))
        out.append(pltpu.roll(u, LANES - 32 * q, 1) if q else u)
    return out


def pack(coef_ref, bands_ref, wh_hbm, wl_hbm, one_ref, two_ref, cbuf, buf, wh_ref, wl_ref, spec, sems):
    halves = [pl.ds(h * LANES, LANES) for h in range(2)]
    mine = lax.axis_index("y")
    turn_by = [lax.rem(k + 4 - mine, 4) for k in range(4)]
    hops = [lax.rem(z + ZD - lax.axis_index("z"), ZD) for z in range(ZD)]
    starts = [pltpu.make_async_copy(coef_ref.at[:, halves[h]], cbuf.at[h], sems.at[h]) for h in range(2)]
    starts += [
        pltpu.make_async_copy(wh_hbm, wh_ref, sems.at[2 + 2 * BANDS]),
        pltpu.make_async_copy(wl_hbm, wl_ref, sems.at[3 + 2 * BANDS]),
    ]
    copies = [
        [pltpu.make_async_copy(bands_ref.at[b, :, halves[h]], buf.at[b, h], sems.at[2 + 2 * b + h]) for h in range(2)]
        for b in range(BANDS)
    ]
    for copy in starts + sum(copies, []):
        copy.start()

    def turn(b):
        for xh in range(2):
            for yh in range(2):
                block = jnp.concatenate(
                    [buf[b, xh, pl.ds(yh * 4 + turn_by[k], ZL, stride=YL), :] for k in range(4)]
                )
                turned = block.T
                for r in range(16):
                    hop, place = hops[xh * 4 + r // 4], r % 4 * COLS + b
                    value = turned[r * 8 : r * 8 + 8]
                    if yh == 0:
                        one_ref[pl.ds(pl.multiple_of(hop * PIECE + place * 8, 8), 8), :] = value
                    else:
                        two_ref[pl.ds(pl.multiple_of(place * SLOT + hop * 8, 8), 8), :] = value

    for step, bands in enumerate(STEPS):
        for b in bands:
            for copy in copies[b]:
                copy.wait()
        if step == DFT_AT:
            for copy in starts:
                copy.wait()
            rows = [
                jnp.concatenate(
                    [cbuf[h, pl.ds(part * N + y // 4 * 4 + turn_by[y % 4], ZL, stride=YL), :] for h in range(2)],
                    axis=1,
                )
                for part in range(2)
                for y in range(YL)
            ]
            q = product(wh_ref[...], wl_ref[...], jnp.concatenate(rows), ((1,), (1,)))
            for h in range(2):
                one, two = (slice(p * N + h * LANES, p * N + (h + 1) * LANES) for p in range(2))
                spec[h, pl.ds(0, N), :] = q[:N, one] - q[N:, two]
                spec[h, pl.ds(N, N), :] = q[N:, one] + q[:N, two]
        for b in bands:
            turn(b)
    for b in range(BANDS):
        for yh in range(2):
            for z in range(ZD):
                for part in range(2):
                    value = spec[yh, pl.ds(part * N + z * 32 + b, 4, stride=8), :]
                    if part == 0:
                        one_ref[pl.ds(hops[z] * PIECE + 8 * PLANE + yh * PLANE + b, 4, stride=COLS), :] = value
                    else:
                        two_ref[pl.ds(b * SLOT + 8 * ZD + hops[z] * 2 + yh, 4, stride=COLS * SLOT), :] = value


STEPS = ((0, 1, 2, 3), (4, 5, 6, 7))
DFT_AT = 0


def regroup(in_ref, *out_refs):
    for k, out_ref in enumerate(out_refs):
        for p in range(PLANE):
            out_ref[pl.ds(p * 8, 8), :] = in_ref[pl.ds(p * SLOT + k * 8, 8), :]
        for j in range(2):
            for g in range(PLANE // 8):
                out_ref[pl.ds(PLANE * 8 + j * PLANE + g * 8, 8), :] = in_ref[
                    pl.ds(g * 8 * SLOT + 8 * ZD + k * 2 + j, 8, stride=SLOT), :
                ]


def join(*refs):
    *in_refs, out_ref = refs
    for k, in_ref in enumerate(in_refs):
        for p in range(PLANE):
            out_ref[pl.ds(p * SLOT + k * 8, 8), :] = in_ref[pl.ds(p * 8, 8), :]
        for j in range(2):
            for g in range(PLANE // 8):
                out_ref[pl.ds(g * 8 * SLOT + 8 * ZD + k * 2 + j, 8, stride=SLOT), :] = in_ref[
                    pl.ds(PLANE * 8 + j * PLANE + g * 8, 8), :
                ]


def unpack(*refs):
    one_ref, *two_refs = refs[: ZD + 1]
    tables_hbm, (coefs_ref, table_ref, *held, cout, tab, field, sems) = refs[ZD + 1 : ZD + 5], refs[ZD + 5 :]
    yh_ref, yl_ref, wh_ref, wl_ref = held
    fetches = [
        pltpu.make_async_copy(source, target, sems.at[2 * ZD + 1 + i])
        for i, (source, target) in enumerate(zip(tables_hbm, held))
    ]
    for fetch in fetches:
        fetch.start()
    flat = tab.reshape(2, XL * (N + 8), LANES)
    source = [lax.rem(lax.axis_index("z") + ZD - k, ZD) for k in range(ZD)]
    for k in range(ZD):
        for part in range(2):
            for yh in range(2):
                for h in range(2):
                    if part == 0:
                        first = h * 4 * SLOT + 8 * ZD + k * 2 + yh
                        vs = [one_ref[pl.ds(first + c * SLOT, 4, stride=COLS * SLOT), :] for c in range(4)]
                    else:
                        first = PLANE * 8 + yh * PLANE + h * 4
                        vs = [two_refs[k][pl.ds(first + c, 4, stride=COLS), :] for c in range(4)]
                    for y, v in enumerate(exchange_blocks(vs)):
                        field[h, pl.ds(part * N + source[k] * 8 + yh * 4 + y, 4, stride=64), :] = v
    for fetch in fetches:
        fetch.wait()
    values = jnp.concatenate([field[0], field[1]], axis=1)
    q = product(yh_ref[...], yl_ref[...], jnp.concatenate([values[:N], values[N:]], axis=1), ((1,), (0,)))
    along = jnp.concatenate([q[:N, :N] - q[N:, N:], q[N:, :N] + q[:N, N:]])
    q = product(wh_ref[...], wl_ref[...], along, ((1,), (1,)))
    real = q[:N, :N] - q[N:, N:]
    imag = q[N:, :N] + q[:N, N:]
    for h in range(2):
        lanes = slice(h * LANES, (h + 1) * LANES)
        cout[pl.ds(h, N, stride=2), :] = real[:, lanes]
        cout[pl.ds(2 * N + h, N, stride=2), :] = imag[:, lanes]
    copies = [pltpu.make_async_copy(cout, coefs_ref, sems.at[2 * ZD])]
    copies[0].start()
    for k in range(ZD):
        for h in range(2):
            for r in range(4):
                for yh in range(2):
                    places = [r * COLS + h * 4 + c for c in range(4)]
                    if yh == 0:
                        vs = [one_ref[pl.ds(p * SLOT + k * 8, 8), :] for p in places]
                    else:
                        vs = [two_refs[k][pl.ds(p * 8, 8), :] for p in places]
                    for y, v in enumerate(exchange_blocks(vs)):
                        flat[h, pl.ds(source[k] * 32 + r * 8 + yh * 4 + y, XL, stride=N + 8), :] = v
            where = pl.ds(pl.multiple_of(source[k] * 32, 32), 32)
            copies.append(
                pltpu.make_async_copy(
                    tab.at[h, :, where, :], table_ref.at[:, where, pl.ds(h * LANES, LANES)], sems.at[2 * k + h]
                )
            )
            copies[-1].start()
    for copy in copies:
        copy.wait()


vmem = pl.BlockSpec(memory_space=pltpu.VMEM)
anywhere = pl.BlockSpec(memory_space=pltpu.HBM)
plane = ("xh", "core", "xl", "y")


def by_hop(values):
    shift = [[(z, (z + k) % ZD) for z in range(ZD)] for k in range(ZD)]
    out = [values[0]] + [None] * (ZD - 1)
    for k in HOPS:
        out[k] = lax.ppermute(values[k], "z", shift[k])
    return out


HOPS = (3, 5, 4, 2, 6, 1, 7)


def local(coefficients, real_bands):
    assert coefficients.shape == (2, 1, ZL, YL, N)
    assert real_bands.shape == (BANDS, ZL, YL, N)
    wh, wl, yh, yl = (jnp.asarray(t) for t in tables())
    params = pltpu.CompilerParams(vmem_limit_bytes=16 << 20)
    one, two = pl.pallas_call(
        pack,
        name="pack",
        out_shape=[
            jax.ShapeDtypeStruct((ZD * PIECE, LANES), f32),
            jax.ShapeDtypeStruct((PLANE * SLOT, LANES), f32),
        ],
        in_specs=[anywhere] * 4,
        out_specs=[vmem, vmem],
        scratch_shapes=[
            pltpu.VMEM((2, 2 * ZL * YL, LANES), f32),
            pltpu.VMEM((BANDS, 2, ZL * YL, LANES), f32),
            pltpu.VMEM((2 * N, N), bf16),
            pltpu.VMEM((2 * N, N), bf16),
            pltpu.VMEM((2, 2 * N, LANES), f32),
            pltpu.SemaphoreType.DMA((4 + 2 * BANDS,)),
        ],
        compiler_params=params,
    )(
        pltpu.with_memory_space_constraint(coefficients.reshape(2 * ZL * YL, N), pltpu.HBM),
        pltpu.with_memory_space_constraint(real_bands.reshape(BANDS, ZL * YL, N), pltpu.HBM),
        pltpu.with_memory_space_constraint(wh, pltpu.HBM),
        pltpu.with_memory_space_constraint(wl, pltpu.HBM),
    )
    two = lax.all_to_all(two.reshape(PLANE, SLOT, LANES), plane, split_axis=0, concat_axis=0, tiled=True)
    one = one.reshape(ZD, PIECE, LANES)
    one = by_hop([one[k] for k in range(ZD)])
    parts = pl.pallas_call(
        regroup,
        name="regroup",
        out_shape=[jax.ShapeDtypeStruct((PIECE, LANES), f32)] * ZD,
        in_specs=[vmem],
        out_specs=[vmem] * ZD,
        compiler_params=params,
    )(two.reshape(PLANE * SLOT, LANES))
    parts = by_hop(parts)
    one = pl.pallas_call(
        join,
        name="join",
        out_shape=jax.ShapeDtypeStruct((ZD * PIECE, LANES), f32),
        in_specs=[vmem] * ZD,
        out_specs=vmem,
        compiler_params=params,
    )(*one)
    one = one.reshape(PLANE, SLOT, LANES)
    one = lax.all_to_all(one, plane, split_axis=0, concat_axis=0, tiled=True)
    coefs, table = pl.pallas_call(
        unpack,
        name="unpack",
        out_shape=[
            jax.ShapeDtypeStruct((4 * N, LANES), f32),
            jax.ShapeDtypeStruct((XL, N, N), f32),
        ],
        in_specs=[vmem] * (ZD + 1) + [anywhere] * 4,
        out_specs=[anywhere, anywhere],
        scratch_shapes=[
            *[pltpu.VMEM((2 * N, N), bf16)] * 4,
            pltpu.VMEM((4 * N, LANES), f32),
            pltpu.VMEM((2, XL, N + 8, LANES), f32),
            pltpu.VMEM((2, 2 * N, LANES), f32),
            pltpu.SemaphoreType.DMA((2 * ZD + 5,)),
        ],
        compiler_params=params,
    )(
        one.reshape(PLANE * SLOT, LANES),
        *parts,
        *[pltpu.with_memory_space_constraint(t, pltpu.HBM) for t in (yh, yl, wh, wl)],
    )
    return coefs.reshape(2, 1, N, 1, N), table.reshape(1, XL, N, N)


def solution(mesh):
    split = jax.sharding.Mesh(mesh.devices.reshape(ZD, 2, 2, 2, 4), ("z", "xh", "core", "xl", "y"))
    row, col = ("z", "xh", "core"), ("xl", "y")
    return jax.shard_map(
        local,
        mesh=split,
        in_specs=(P(None, None, col, row, None), P(None, col, row, None)),
        out_specs=(P(None, None, None, row + col, None), P(col, row, None, None)),
        check_vma=False,
    )
```

```python
import functools

import jax
import jax.numpy as jnp
import ml_dtypes
import numpy as np
from jax import lax
from jax.experimental import pallas as pl
from jax.experimental.pallas import tpu as pltpu
from jax.sharding import PartitionSpec as P

N = 256
ROWS, COLS = 32, 8
ZL, YL, XL = N // COLS, N // ROWS, N // ROWS
BANDS = 8
ZD, PLANE = 8, 32
PIECE = 10 * PLANE
SLOT = 10 * ZD
LANES = 128
f32 = jnp.float32
bf16 = jnp.bfloat16


@functools.cache
def tables():
    k = np.arange(N)
    angle = 2.0 * np.pi * ((k[:, None] * k[None, :]) % N) / N
    weight = 6.0 / ((4.0 + 2.0 * np.cos(2.0 * np.pi * k / N)) * np.sqrt(N))
    both = np.concatenate([np.cos(angle) * weight[None, :], np.sin(angle) * weight[None, :]])
    by_rest = both.reshape(2 * N, ZD, ROWS // ZD, YL).swapaxes(1, 2).reshape(2 * N, N)
    out = []
    for whole in (both, by_rest):
        high = whole.astype(ml_dtypes.bfloat16)
        low = (whole - high.astype(np.float64)).astype(ml_dtypes.bfloat16)
        out += [high, low]
    return tuple(out)


def split(value):
    high = value.astype(bf16)
    return high, (value - high.astype(f32)).astype(bf16)


def product(w_high, w_low, value, dims):
    high, low = split(value)

    def one(left, right):
        return lax.dot_general(left, right, (dims, ((), ())), preferred_element_type=f32)

    return one(w_high, high) + (one(w_high, low) + one(w_low, high))


def exchange_blocks(vs):
    lane = lax.broadcasted_iota(jnp.int32, vs[0].shape, 1)
    low = lane < 64
    even = (lane & 32) == 0
    out = []
    for q in range(4):
        a, b, c, d = (vs[(place - q) % 4] for place in range(4))
        u = jnp.where(low, jnp.where(even, a, b), jnp.where(even, c, d))
        out.append(pltpu.roll(u, LANES - 32 * q, 1) if q else u)
    return out


def pack(coef_ref, bands_ref, wh_hbm, wl_hbm, *refs):
    out_one, out_two, (one_ref, two_ref, cbuf, buf, wh_ref, wl_ref, spec, sems) = refs[:ZD], refs[ZD], refs[ZD + 1 :]
    halves = [pl.ds(h * LANES, LANES) for h in range(2)]
    mine = lax.axis_index("y")
    turn_by = [lax.rem(k + 4 - mine, 4) for k in range(4)]
    hops = [lax.rem(z + ZD - lax.axis_index("z"), ZD) for z in range(ZD)]
    starts = [pltpu.make_async_copy(coef_ref.at[:, halves[h]], cbuf.at[h], sems.at[h]) for h in range(2)]
    starts += [
        pltpu.make_async_copy(wh_hbm, wh_ref, sems.at[2 + 2 * BANDS]),
        pltpu.make_async_copy(wl_hbm, wl_ref, sems.at[3 + 2 * BANDS]),
    ]
    copies = [
        [pltpu.make_async_copy(bands_ref.at[b, :, halves[h]], buf.at[b, h], sems.at[2 + 2 * b + h]) for h in range(2)]
        for b in range(BANDS)
    ]
    for copy in starts + sum(copies, []):
        copy.start()

    def turn(b, yh):
        for xh in range(2):
            block = jnp.concatenate([buf[b, xh, pl.ds(yh * 4 + turn_by[k], ZL, stride=YL), :] for k in range(4)])
            turned = block.T
            for r in range(16):
                hop, place = hops[xh * 4 + r // 4], r % 4 * COLS + b
                value = turned[r * 8 : r * 8 + 8]
                if yh == 0:
                    one_ref[pl.ds(pl.multiple_of(hop * PIECE + place * 8, 8), 8), :] = value
                else:
                    two_ref[pl.ds(pl.multiple_of(place * SLOT + hop * 8, 8), 8), :] = value

    for step, bands in enumerate(STEPS):
        for b in bands:
            for copy in copies[b]:
                copy.wait()
        if step == DFT_AT:
            for copy in starts:
                copy.wait()
            rows = [
                jnp.concatenate(
                    [cbuf[h, pl.ds(part * N + y // 4 * 4 + turn_by[y % 4], ZL, stride=YL), :] for h in range(2)],
                    axis=1,
                )
                for part in range(2)
                for y in range(YL)
            ]
            q = product(wh_ref[...], wl_ref[...], jnp.concatenate(rows), ((1,), (1,)))
            for h in range(2):
                one, two = (slice(p * N + h * LANES, p * N + (h + 1) * LANES) for p in range(2))
                spec[h, pl.ds(0, N), :] = q[:N, one] - q[N:, two]
                spec[h, pl.ds(N, N), :] = q[N:, one] + q[:N, two]
        for b in bands:
            turn(b, 0)
    for b in range(BANDS):
        for yh in range(2):
            for z in range(ZD):
                one_ref[pl.ds(hops[z] * PIECE + 8 * PLANE + yh * PLANE + b, 4, stride=COLS), :] = spec[
                    yh, pl.ds(z * 32 + b, 4, stride=8), :
                ]
    out = [
        pltpu.make_async_copy(one_ref.at[pl.ds(k * PIECE, PIECE)], out_one[k], sems.at[4 + 2 * BANDS + k])
        for k in range(ZD)
    ]
    for copy in out:
        copy.start()
    for b in range(BANDS):
        turn(b, 1)
        for yh in range(2):
            for z in range(ZD):
                two_ref[pl.ds(b * SLOT + 8 * ZD + hops[z] * 2 + yh, 4, stride=COLS * SLOT), :] = spec[
                    yh, pl.ds(N + z * 32 + b, 4, stride=8), :
                ]
    out.append(pltpu.make_async_copy(two_ref, out_two, sems.at[4 + 2 * BANDS + ZD]))
    out[-1].start()
    for copy in out:
        copy.wait()


STEPS = ((0, 1, 2, 3), (4, 5, 6, 7))
DFT_AT = 0


def regroup(in_ref, *refs):
    out_refs, held, sems = refs[:ZD], refs[ZD], refs[ZD + 1]
    late = HOPS[AHEAD:]
    copies = []
    for k in late + tuple(k for k in range(ZD) if k not in late):
        out_ref = held.at[late.index(k)] if k in late else out_refs[k]
        for p in range(PLANE):
            out_ref[pl.ds(p * 8, 8), :] = in_ref[pl.ds(p * SLOT + k * 8, 8), :]
        for j in range(2):
            for g in range(PLANE // 8):
                out_ref[pl.ds(PLANE * 8 + j * PLANE + g * 8, 8), :] = in_ref[
                    pl.ds(g * 8 * SLOT + 8 * ZD + k * 2 + j, 8, stride=SLOT), :
                ]
        if k in late:
            copies.append(pltpu.make_async_copy(out_ref, out_refs[k], sems.at[late.index(k)]))
            copies[-1].start()
    for copy in copies:
        copy.wait()


def join(*refs):
    *in_refs, out_ref = refs
    for k, in_ref in enumerate(in_refs):
        for p in range(PLANE):
            out_ref[pl.ds(p * SLOT + k * 8, 8), :] = in_ref[pl.ds(p * 8, 8), :]
        for j in range(2):
            for g in range(PLANE // 8):
                out_ref[pl.ds(g * 8 * SLOT + 8 * ZD + k * 2 + j, 8, stride=SLOT), :] = in_ref[
                    pl.ds(PLANE * 8 + j * PLANE + g * 8, 8), :
                ]


BEFORE = 6


def unpack(*refs):
    one_ref, *two_refs = refs[: ZD + 1]
    tables_hbm, (coefs_ref, table_ref, *held, cout, tab, field, sems) = refs[ZD + 1 : ZD + 5], refs[ZD + 5 :]
    yh_ref, yl_ref, wh_ref, wl_ref = held
    fetches = [
        pltpu.make_async_copy(source, target, sems.at[2 * ZD + 1 + i])
        for i, (source, target) in enumerate(zip(tables_hbm, held))
    ]
    for fetch in fetches:
        fetch.start()
    flat = tab.reshape(2, XL * (N + 8), LANES)
    source = [lax.rem(lax.axis_index("z") + ZD - k, ZD) for k in range(ZD)]
    for k in range(ZD):
        for part in range(2):
            for yh in range(2):
                if part == 0:
                    vs = [one_ref[pl.ds(c * SLOT + 8 * ZD + k * 2 + yh, 8, stride=4 * SLOT), :] for c in range(4)]
                else:
                    vs = [two_refs[k][pl.ds(PLANE * 8 + yh * PLANE + c, 8, stride=4), :] for c in range(4)]
                for y, v in enumerate(exchange_blocks(vs)):
                    field[pl.ds(part * 2 * N + source[k] * 8 + yh * 4 + y, 8, stride=64), :] = v
    copies = []

    def place(k):
        for h in range(2):
            for r in range(4):
                for yh in range(2):
                    places = [r * COLS + h * 4 + c for c in range(4)]
                    if yh == 0:
                        vs = [one_ref[pl.ds(p * SLOT + k * 8, 8), :] for p in places]
                    else:
                        vs = [two_refs[k][pl.ds(p * 8, 8), :] for p in places]
                    for y, v in enumerate(exchange_blocks(vs)):
                        flat[h, pl.ds(source[k] * 32 + r * 8 + yh * 4 + y, XL, stride=N + 8), :] = v
            where = pl.ds(pl.multiple_of(source[k] * 32, 32), 32)
            copies.append(
                pltpu.make_async_copy(
                    tab.at[h, :, where, :], table_ref.at[:, where, pl.ds(h * LANES, LANES)], sems.at[2 * k + h]
                )
            )
            copies[-1].start()

    for k in range(BEFORE):
        place(k)
    for fetch in fetches:
        fetch.wait()
    values = jnp.concatenate(
        [
            jnp.concatenate([field[pl.ds(part * 2 * N + r * 128 + h * 64, 64), :] for r in range(4)])
            for part in range(2)
            for h in range(2)
        ],
        axis=1,
    )
    q = product(yh_ref[...], yl_ref[...], values, ((1,), (0,)))
    along = jnp.concatenate([q[:N, :N] - q[N:, N:], q[N:, :N] + q[:N, N:]])
    q = product(wh_ref[...], wl_ref[...], along, ((1,), (1,)))
    real = q[:N, :N] - q[N:, N:]
    imag = q[N:, :N] + q[:N, N:]
    for h in range(2):
        lanes = slice(h * LANES, (h + 1) * LANES)
        cout[pl.ds(h, N, stride=2), :] = real[:, lanes]
        cout[pl.ds(2 * N + h, N, stride=2), :] = imag[:, lanes]
    copies.append(pltpu.make_async_copy(cout, coefs_ref, sems.at[2 * ZD]))
    copies[-1].start()
    for k in range(BEFORE, ZD):
        place(k)
    for copy in copies:
        copy.wait()


vmem = pl.BlockSpec(memory_space=pltpu.VMEM)
anywhere = pl.BlockSpec(memory_space=pltpu.HBM)
plane = ("xh", "core", "xl", "y")


def by_hop(values):
    shift = [[(z, (z + k) % ZD) for z in range(ZD)] for k in range(ZD)]
    out = [values[0]] + [None] * (ZD - 1)
    for k in HOPS:
        out[k] = lax.ppermute(values[k], "z", shift[k])
    return out


HOPS = (3, 5, 4, 2, 6, 1, 7)
AHEAD = 3


def local(coefficients, real_bands):
    assert coefficients.shape == (2, 1, ZL, YL, N)
    assert real_bands.shape == (BANDS, ZL, YL, N)
    wh, wl, yh, yl = (jnp.asarray(t) for t in tables())
    params = pltpu.CompilerParams(vmem_limit_bytes=16 << 20)
    *one, two = pl.pallas_call(
        pack,
        name="pack",
        out_shape=[jax.ShapeDtypeStruct((PIECE, LANES), f32)] * ZD + [jax.ShapeDtypeStruct((PLANE * SLOT, LANES), f32)],
        in_specs=[anywhere] * 4,
        out_specs=[anywhere] * (ZD + 1),
        scratch_shapes=[
            pltpu.VMEM((ZD * PIECE, LANES), f32),
            pltpu.VMEM((PLANE * SLOT, LANES), f32),
            pltpu.VMEM((2, 2 * ZL * YL, LANES), f32),
            pltpu.VMEM((BANDS, 2, ZL * YL, LANES), f32),
            pltpu.VMEM((2 * N, N), bf16),
            pltpu.VMEM((2 * N, N), bf16),
            pltpu.VMEM((2, 2 * N, LANES), f32),
            pltpu.SemaphoreType.DMA((5 + 2 * BANDS + ZD,)),
        ],
        compiler_params=params,
    )(
        pltpu.with_memory_space_constraint(coefficients.reshape(2 * ZL * YL, N), pltpu.HBM),
        pltpu.with_memory_space_constraint(real_bands.reshape(BANDS, ZL * YL, N), pltpu.HBM),
        pltpu.with_memory_space_constraint(wh, pltpu.HBM),
        pltpu.with_memory_space_constraint(wl, pltpu.HBM),
    )
    two = lax.all_to_all(two.reshape(PLANE, SLOT, LANES), plane, split_axis=0, concat_axis=0, tiled=True)
    one = by_hop(one)
    parts = pl.pallas_call(
        regroup,
        name="regroup",
        out_shape=[(pltpu.HBM if k in HOPS[AHEAD:] else pltpu.VMEM)((PIECE, LANES), f32) for k in range(ZD)],
        in_specs=[vmem],
        out_specs=[anywhere if k in HOPS[AHEAD:] else vmem for k in range(ZD)],
        scratch_shapes=[
            pltpu.VMEM((len(HOPS) - AHEAD, PIECE, LANES), f32),
            pltpu.SemaphoreType.DMA((len(HOPS) - AHEAD,)),
        ],
        compiler_params=params,
    )(two.reshape(PLANE * SLOT, LANES))
    parts = by_hop(parts)
    one = pl.pallas_call(
        join,
        name="join",
        out_shape=jax.ShapeDtypeStruct((ZD * PIECE, LANES), f32),
        in_specs=[vmem] * ZD,
        out_specs=vmem,
        compiler_params=params,
    )(*one)
    one = one.reshape(PLANE, SLOT, LANES)
    one = lax.all_to_all(one, plane, split_axis=0, concat_axis=0, tiled=True)
    coefs, table = pl.pallas_call(
        unpack,
        name="unpack",
        out_shape=[
            jax.ShapeDtypeStruct((4 * N, LANES), f32),
            jax.ShapeDtypeStruct((XL, N, N), f32),
        ],
        in_specs=[vmem] * (ZD + 1) + [anywhere] * 4,
        out_specs=[anywhere, anywhere],
        scratch_shapes=[
            *[pltpu.VMEM((2 * N, N), bf16)] * 4,
            pltpu.VMEM((4 * N, LANES), f32),
            pltpu.VMEM((2, XL, N + 8, LANES), f32),
            pltpu.VMEM((4 * N, LANES), f32),
            pltpu.SemaphoreType.DMA((2 * ZD + 5,)),
        ],
        compiler_params=params,
    )(
        one.reshape(PLANE * SLOT, LANES),
        *parts,
        *[pltpu.with_memory_space_constraint(t, pltpu.HBM) for t in (yh, yl, wh, wl)],
    )
    return coefs.reshape(2, 1, N, 1, N), table.reshape(1, XL, N, N)


def solution(mesh):
    split = jax.sharding.Mesh(mesh.devices.reshape(ZD, 2, 2, 2, 4), ("z", "xh", "core", "xl", "y"))
    row, col = ("z", "xh", "core"), ("xl", "y")
    return jax.shard_map(
        local,
        mesh=split,
        in_specs=(P(None, None, col, row, None), P(None, col, row, None)),
        out_specs=(P(None, None, None, row + col, None), P(col, row, None, None)),
        check_vma=False,
    )
```

```python
import functools

import jax
import jax.numpy as jnp
import ml_dtypes
import numpy as np
from jax import lax
from jax.experimental import pallas as pl
from jax.experimental.pallas import tpu as pltpu
from jax.sharding import PartitionSpec as P

N = 256
ROWS, COLS = 32, 8
ZL, YL, XL = N // COLS, N // ROWS, N // ROWS
BANDS = 8
ZD, PLANE = 8, 32
PIECE = 10 * PLANE
SLOT = 10 * ZD
LANES = 128
f32 = jnp.float32
bf16 = jnp.bfloat16


@functools.cache
def tables():
    k = np.arange(N)
    angle = 2.0 * np.pi * ((k[:, None] * k[None, :]) % N) / N
    weight = 6.0 / ((4.0 + 2.0 * np.cos(2.0 * np.pi * k / N)) * np.sqrt(N))
    both = np.concatenate([np.cos(angle) * weight[None, :], np.sin(angle) * weight[None, :]])
    by_rest = both.reshape(2 * N, ZD, ROWS // ZD, YL).swapaxes(1, 2).reshape(2 * N, N)
    out = []
    for whole in (both, by_rest):
        high = whole.astype(ml_dtypes.bfloat16)
        low = (whole - high.astype(np.float64)).astype(ml_dtypes.bfloat16)
        out += [high, low]
    return tuple(out)


def split(value):
    high = value.astype(bf16)
    return high, (value - high.astype(f32)).astype(bf16)


def product(w_high, w_low, value, dims):
    high, low = split(value)

    def one(left, right):
        return lax.dot_general(left, right, (dims, ((), ())), preferred_element_type=f32)

    return one(w_high, high) + (one(w_high, low) + one(w_low, high))


def exchange_blocks(vs):
    lane = lax.broadcasted_iota(jnp.int32, vs[0].shape, 1)
    low = lane < 64
    even = (lane & 32) == 0
    out = []
    for q in range(4):
        a, b, c, d = (vs[(place - q) % 4] for place in range(4))
        u = jnp.where(low, jnp.where(even, a, b), jnp.where(even, c, d))
        out.append(pltpu.roll(u, LANES - 32 * q, 1) if q else u)
    return out


def pack(coef_ref, bands_ref, wh_hbm, wl_hbm, *refs):
    out_one, out_two, (one_ref, two_ref, cbuf, buf, wh_ref, wl_ref, spec, sems) = refs[:ZD], refs[ZD], refs[ZD + 1 :]
    halves = [pl.ds(h * LANES, LANES) for h in range(2)]
    mine = lax.axis_index("y")
    turn_by = [lax.rem(k + 4 - mine, 4) for k in range(4)]
    hops = [lax.rem(z + ZD - lax.axis_index("z"), ZD) for z in range(ZD)]
    starts = [pltpu.make_async_copy(coef_ref.at[:, halves[h]], cbuf.at[h], sems.at[h]) for h in range(2)]
    starts += [
        pltpu.make_async_copy(wh_hbm, wh_ref, sems.at[2 + 2 * BANDS]),
        pltpu.make_async_copy(wl_hbm, wl_ref, sems.at[3 + 2 * BANDS]),
    ]
    copies = [
        [pltpu.make_async_copy(bands_ref.at[b, :, halves[h]], buf.at[b, h], sems.at[2 + 2 * b + h]) for h in range(2)]
        for b in range(BANDS)
    ]
    for copy in starts + sum(copies, []):
        copy.start()

    def turn(b, yh):
        for xh in range(2):
            block = jnp.concatenate([buf[b, xh, pl.ds(yh * 4 + turn_by[k], ZL, stride=YL), :] for k in range(4)])
            turned = block.T
            for r in range(16):
                hop, place = hops[xh * 4 + r // 4], r % 4 * COLS + b
                value = turned[r * 8 : r * 8 + 8]
                if yh == 0:
                    one_ref[pl.ds(pl.multiple_of(hop * PIECE + place * 8, 8), 8), :] = value
                else:
                    two_ref[pl.ds(pl.multiple_of(place * SLOT + hop * 8, 8), 8), :] = value

    for step, bands in enumerate(STEPS):
        for b in bands:
            for copy in copies[b]:
                copy.wait()
        if step == DFT_AT:
            for copy in starts:
                copy.wait()
            rows = [
                jnp.concatenate(
                    [cbuf[h, pl.ds(part * N + y // 4 * 4 + turn_by[y % 4], ZL, stride=YL), :] for h in range(2)],
                    axis=1,
                )
                for part in range(2)
                for y in range(YL)
            ]
            q = product(wh_ref[...], wl_ref[...], jnp.concatenate(rows), ((1,), (1,)))
            for h in range(2):
                one, two = (slice(p * N + h * LANES, p * N + (h + 1) * LANES) for p in range(2))
                spec[h, pl.ds(0, N), :] = q[:N, one] - q[N:, two]
                spec[h, pl.ds(N, N), :] = q[N:, one] + q[:N, two]
        for b in bands:
            turn(b, 0)
    for z in range(ZD):
        for yh in range(2):
            for r in range(4):
                row = hops[z] * PIECE + 8 * PLANE + yh * PLANE + r * 8
                one_ref[pl.ds(pl.multiple_of(row, 8), 8), :] = spec[yh, pl.ds(z * 32 + r * 8, 8), :]
    out = [
        pltpu.make_async_copy(one_ref.at[pl.ds(k * PIECE, PIECE)], out_one[k], sems.at[4 + 2 * BANDS + k])
        for k in range(ZD)
    ]
    for copy in out:
        copy.start()
    for z in range(ZD):
        for yh in range(2):
            for r in range(4):
                two_ref[pl.ds(r * COLS * SLOT + 8 * ZD + hops[z] * 2 + yh, 8, stride=SLOT), :] = spec[
                    yh, pl.ds(N + z * 32 + r * 8, 8), :
                ]
    for b in range(BANDS):
        turn(b, 1)
        for r in range(4):
            where = pl.ds((r * COLS + b) * SLOT, SLOT)
            out.append(
                pltpu.make_async_copy(two_ref.at[where], out_two.at[where], sems.at[4 + 2 * BANDS + ZD + 4 * b + r])
            )
            out[-1].start()
    for copy in out:
        copy.wait()


STEPS = ((0, 1, 2, 3), (4, 5, 6, 7))
DFT_AT = 0


def regroup(in_ref, *refs):
    out_refs, held, sems = refs[:ZD], refs[ZD], refs[ZD + 1]
    late = HOPS[AHEAD:]
    copies = []
    for k in late + tuple(k for k in range(ZD) if k not in late):
        out_ref = held.at[late.index(k)] if k in late else out_refs[k]
        for p in range(PLANE):
            out_ref[pl.ds(p * 8, 8), :] = in_ref[pl.ds(p * SLOT + k * 8, 8), :]
        for j in range(2):
            for g in range(PLANE // 8):
                out_ref[pl.ds(PLANE * 8 + j * PLANE + g * 8, 8), :] = in_ref[
                    pl.ds(g * 8 * SLOT + 8 * ZD + k * 2 + j, 8, stride=SLOT), :
                ]
        if k in late:
            copies.append(pltpu.make_async_copy(out_ref, out_refs[k], sems.at[late.index(k)]))
            copies[-1].start()
    for copy in copies:
        copy.wait()


def join(*refs):
    *in_refs, out_ref, held, sems = refs
    copies = []
    for g in range(PLANE // 8):
        for k, in_ref in enumerate(in_refs):
            for p in range(g * 8, g * 8 + 8):
                held[pl.ds(p * SLOT + k * 8, 8), :] = in_ref[pl.ds(p * 8, 8), :]
            for j in range(2):
                held[pl.ds(g * 8 * SLOT + 8 * ZD + k * 2 + j, 8, stride=SLOT), :] = in_ref[
                    pl.ds(PLANE * 8 + j * PLANE + g * 8, 8), :
                ]
        where = pl.ds(g * 8 * SLOT, 8 * SLOT)
        copies.append(pltpu.make_async_copy(held.at[where], out_ref.at[where], sems.at[g]))
        copies[-1].start()
    for copy in copies:
        copy.wait()


BEFORE = 6


def unpack(*refs):
    one_ref, *two_refs = refs[: ZD + 1]
    tables_hbm, (coefs_ref, table_ref, *held, cout, tab, field, sems) = refs[ZD + 1 : ZD + 5], refs[ZD + 5 :]
    yh_ref, yl_ref, wh_ref, wl_ref = held
    fetches = [
        pltpu.make_async_copy(source, target, sems.at[2 * ZD + 1 + i])
        for i, (source, target) in enumerate(zip(tables_hbm, held))
    ]
    for fetch in fetches:
        fetch.start()
    flat = tab.reshape(2, XL * (N + 8), LANES)
    source = [lax.rem(lax.axis_index("z") + ZD - k, ZD) for k in range(ZD)]
    for k in range(ZD):
        for part in range(2):
            for yh in range(2):
                if part == 0:
                    vs = [one_ref[pl.ds(c * SLOT + 8 * ZD + k * 2 + yh, 8, stride=4 * SLOT), :] for c in range(4)]
                else:
                    vs = [two_refs[k][pl.ds(PLANE * 8 + yh * PLANE + c, 8, stride=4), :] for c in range(4)]
                for y, v in enumerate(exchange_blocks(vs)):
                    field[pl.ds(part * 2 * N + source[k] * 8 + yh * 4 + y, 8, stride=64), :] = v
    copies = []

    def place(k):
        for h in range(2):
            for r in range(4):
                for yh in range(2):
                    places = [r * COLS + h * 4 + c for c in range(4)]
                    if yh == 0:
                        vs = [one_ref[pl.ds(p * SLOT + k * 8, 8), :] for p in places]
                    else:
                        vs = [two_refs[k][pl.ds(p * 8, 8), :] for p in places]
                    for y, v in enumerate(exchange_blocks(vs)):
                        flat[h, pl.ds(source[k] * 32 + r * 8 + yh * 4 + y, XL, stride=N + 8), :] = v
            where = pl.ds(pl.multiple_of(source[k] * 32, 32), 32)
            copies.append(
                pltpu.make_async_copy(
                    tab.at[h, :, where, :], table_ref.at[:, where, pl.ds(h * LANES, LANES)], sems.at[2 * k + h]
                )
            )
            copies[-1].start()

    for k in range(BEFORE):
        place(k)
    for fetch in fetches:
        fetch.wait()
    values = jnp.concatenate(
        [
            jnp.concatenate([field[pl.ds(part * 2 * N + r * 128 + h * 64, 64), :] for r in range(4)])
            for part in range(2)
            for h in range(2)
        ],
        axis=1,
    )
    q = product(yh_ref[...], yl_ref[...], values, ((1,), (0,)))
    along = jnp.concatenate([q[:N, :N] - q[N:, N:], q[N:, :N] + q[:N, N:]])
    q = product(wh_ref[...], wl_ref[...], along, ((1,), (1,)))
    real = q[:N, :N] - q[N:, N:]
    imag = q[N:, :N] + q[:N, N:]
    for h in range(2):
        lanes = slice(h * LANES, (h + 1) * LANES)
        cout[pl.ds(h, N, stride=2), :] = real[:, lanes]
        cout[pl.ds(2 * N + h, N, stride=2), :] = imag[:, lanes]
    copies.append(pltpu.make_async_copy(cout, coefs_ref, sems.at[2 * ZD]))
    copies[-1].start()
    for k in range(BEFORE, ZD):
        place(k)
    for copy in copies:
        copy.wait()


vmem = pl.BlockSpec(memory_space=pltpu.VMEM)
anywhere = pl.BlockSpec(memory_space=pltpu.HBM)
plane = ("xh", "core", "xl", "y")


def by_hop(values):
    shift = [[(z, (z + k) % ZD) for z in range(ZD)] for k in range(ZD)]
    out = [values[0]] + [None] * (ZD - 1)
    for k in HOPS:
        out[k] = lax.ppermute(values[k], "z", shift[k])
    return out


HOPS = (3, 5, 4, 2, 6, 1, 7)
AHEAD = 3


def local(coefficients, real_bands):
    assert coefficients.shape == (2, 1, ZL, YL, N)
    assert real_bands.shape == (BANDS, ZL, YL, N)
    wh, wl, yh, yl = (jnp.asarray(t) for t in tables())
    params = pltpu.CompilerParams(vmem_limit_bytes=16 << 20)
    *one, two = pl.pallas_call(
        pack,
        name="pack",
        out_shape=[jax.ShapeDtypeStruct((PIECE, LANES), f32)] * ZD + [jax.ShapeDtypeStruct((PLANE * SLOT, LANES), f32)],
        in_specs=[anywhere] * 4,
        out_specs=[anywhere] * (ZD + 1),
        scratch_shapes=[
            pltpu.VMEM((ZD * PIECE, LANES), f32),
            pltpu.VMEM((PLANE * SLOT, LANES), f32),
            pltpu.VMEM((2, 2 * ZL * YL, LANES), f32),
            pltpu.VMEM((BANDS, 2, ZL * YL, LANES), f32),
            pltpu.VMEM((2 * N, N), bf16),
            pltpu.VMEM((2 * N, N), bf16),
            pltpu.VMEM((2, 2 * N, LANES), f32),
            pltpu.SemaphoreType.DMA((4 + 6 * BANDS + ZD,)),
        ],
        compiler_params=params,
    )(
        pltpu.with_memory_space_constraint(coefficients.reshape(2 * ZL * YL, N), pltpu.HBM),
        pltpu.with_memory_space_constraint(real_bands.reshape(BANDS, ZL * YL, N), pltpu.HBM),
        pltpu.with_memory_space_constraint(wh, pltpu.HBM),
        pltpu.with_memory_space_constraint(wl, pltpu.HBM),
    )
    two = lax.all_to_all(two.reshape(PLANE, SLOT, LANES), plane, split_axis=0, concat_axis=0, tiled=True)
    one = by_hop(one)
    parts = pl.pallas_call(
        regroup,
        name="regroup",
        out_shape=[(pltpu.HBM if k in HOPS[AHEAD:] else pltpu.VMEM)((PIECE, LANES), f32) for k in range(ZD)],
        in_specs=[vmem],
        out_specs=[anywhere if k in HOPS[AHEAD:] else vmem for k in range(ZD)],
        scratch_shapes=[
            pltpu.VMEM((len(HOPS) - AHEAD, PIECE, LANES), f32),
            pltpu.SemaphoreType.DMA((len(HOPS) - AHEAD,)),
        ],
        compiler_params=params,
    )(two.reshape(PLANE * SLOT, LANES))
    parts = by_hop(parts)
    one = pl.pallas_call(
        join,
        name="join",
        out_shape=pltpu.HBM((PLANE * SLOT, LANES), f32),
        in_specs=[vmem] * ZD,
        out_specs=anywhere,
        scratch_shapes=[
            pltpu.VMEM((PLANE * SLOT, LANES), f32),
            pltpu.SemaphoreType.DMA((PLANE // 8,)),
        ],
        compiler_params=params,
    )(*one)
    one = one.reshape(PLANE, SLOT, LANES)
    one = lax.all_to_all(one, plane, split_axis=0, concat_axis=0, tiled=True)
    coefs, table = pl.pallas_call(
        unpack,
        name="unpack",
        out_shape=[
            jax.ShapeDtypeStruct((4 * N, LANES), f32),
            jax.ShapeDtypeStruct((XL, N, N), f32),
        ],
        in_specs=[vmem] * (ZD + 1) + [anywhere] * 4,
        out_specs=[anywhere, anywhere],
        scratch_shapes=[
            *[pltpu.VMEM((2 * N, N), bf16)] * 4,
            pltpu.VMEM((4 * N, LANES), f32),
            pltpu.VMEM((2, XL, N + 8, LANES), f32),
            pltpu.VMEM((4 * N, LANES), f32),
            pltpu.SemaphoreType.DMA((2 * ZD + 5,)),
        ],
        compiler_params=params,
    )(
        one.reshape(PLANE * SLOT, LANES),
        *parts,
        *[pltpu.with_memory_space_constraint(t, pltpu.HBM) for t in (yh, yl, wh, wl)],
    )
    return coefs.reshape(2, 1, N, 1, N), table.reshape(1, XL, N, N)


def solution(mesh):
    split = jax.sharding.Mesh(mesh.devices.reshape(ZD, 2, 2, 2, 4), ("z", "xh", "core", "xl", "y"))
    row, col = ("z", "xh", "core"), ("xl", "y")
    return jax.shard_map(
        local,
        mesh=split,
        in_specs=(P(None, None, col, row, None), P(None, col, row, None)),
        out_specs=(P(None, None, None, row + col, None), P(col, row, None, None)),
        check_vma=False,
    )
```
